32 devices in a mesh: dp: 16 (over z, y, x), mp: 2 (over core).
Axes of the slice: x: 2, y: 2, z: 4, core: 2. Of those that a mesh axis runs over, the one named last changes fastest.
Arguments:
- belief: bfloat16 [4096, 2652], P('dp'), may hold values from -6 to 6
- target_value: bfloat16 [4096, 1326], P('dp'), may hold values from -6 to 6
- counts: int32 [32], P('dp'), may hold values from 1 to 128, as said below
- w_first: bfloat16 [2652, 1536], P(None, 'mp'), may hold values from -0.125 to 0.125
- w_middle: bfloat16 [1536, 1536], P('mp'), may hold values from -0.15625 to 0.15625
- w_last: bfloat16 [1536, 1326], P(None, 'mp'), may hold values from -0.15625 to 0.15625
Outputs:
- grad_first: float32 [2652, 1536], P(None, ('mp', 'dp'))
- grad_middle: float32 [1536, 1536], P('mp', 'dp')
- grad_last: float32 [1536, 1326], P('dp', 'mp')
The draws below stay inside these ranges and needn't reach their ends.
Inputs may be any that keep to these rules, and one draw needn't show every extreme that they name: `counts`: rows past a subgame's count in its block are padding with arbitrary values.
All inputs are finite; a program needn't handle non-finite values.
Results may differ from the reference program's by a relative error of at most 0.0089.
Values may be sent and summed in bfloat16 or wider, within the bound.
A program may use at most 192 MiB of HBM per device.

```python
import jax
import jax.numpy as jnp
from jax import lax

IN = 2652
HID = 1536
OUT = 1326
BLOCK = 128
SUB_DEV = 2
ROWS = 4096
PARAMS = 8469504
N_DP = 16


def draw_counts(key, part):
    key_ceiling, key_counts, key_spot = jax.random.split(key, 3)
    ceiling = jax.random.randint(key_ceiling, (N_DP, 1), 48, BLOCK + 1)
    floor_level = ceiling // 2
    drawn = jax.random.randint(key_counts, (N_DP, SUB_DEV), floor_level, ceiling + 1)
    flat_counts = drawn.reshape(N_DP * SUB_DEV)
    spot = jax.random.randint(key_spot, (), 0, N_DP * SUB_DEV)
    return flat_counts.at[spot].set(BLOCK).astype(jnp.int32)


def steps_of(key, shape, shards, least, high):
    level = 1.0
    for position, parts in shards:
        steps = jax.random.uniform(jax.random.fold_in(jax.random.fold_in(key, 6), position), (parts,), jnp.float32, least / len(shards), high / len(shards))
        level = level * jnp.repeat(jnp.exp(steps), shape[position] // parts).reshape((-1,) + (1,) * (len(shape) - 1 - position))
    return level


def scatter_about(own_key, shape, scale, reach, cuts=(), kind=jnp.bfloat16):
    factor_of = steps_of(own_key, shape, cuts, -0.22, 0.18) if cuts else 1.0
    values = jax.random.normal(own_key, shape, jnp.float32) * scale * factor_of
    return jnp.minimum(jnp.maximum(values, -reach), reach).astype(kind)


def setup_inputs(seed: int = 0) -> dict:
    key_of = jax.random.split(jax.random.key(seed), 7)
    return {
        "belief": scatter_about(key_of[0], (ROWS, IN), 1.0, 6.0, ((0, 16),)),
        "target_value": scatter_about(key_of[1], (ROWS, OUT), 1.0, 6.0, ((0, 16),)),
        "counts": draw_counts(jax.random.fold_in(key_of[6], 71), 0),
        "w_first": scatter_about(key_of[3], (IN, HID), IN ** -0.5, 0.125, ((1, 2),)),
        "w_middle": scatter_about(key_of[4], (HID, HID), HID ** -0.5, 0.15625, ((0, 2),)),
        "w_last": scatter_about(key_of[5], (HID, OUT), HID ** -0.5, 0.15625, ((1, 2),)),
    }


def silu_slope(pre_act):
    sigmoid_of = jax.nn.sigmoid(pre_act)
    return sigmoid_of * (1.0 + pre_act * (1.0 - sigmoid_of))

def rows_grads(belief, target_value, live_mask, w_first, w_middle, w_last):
    pre_first = jnp.dot(belief, w_first, preferred_element_type=jnp.float32)
    act_first = jax.nn.silu(pre_first).astype(jnp.bfloat16)
    pre_middle = jnp.dot(act_first, w_middle, preferred_element_type=jnp.float32)
    act_middle = jax.nn.silu(pre_middle).astype(jnp.bfloat16)
    predicted = jnp.dot(act_middle, w_last, preferred_element_type=jnp.float32)
    mismatch = predicted - target_value.astype(jnp.float32)
    slope_out = (jnp.clip(mismatch, -1.0, 1.0) * live_mask[:, None]).astype(jnp.bfloat16)
    raw_last = jnp.dot(act_middle.T, slope_out, preferred_element_type=jnp.float32)
    back_middle = jnp.dot(slope_out, w_last.T, preferred_element_type=jnp.float32)
    slope_middle = (back_middle * silu_slope(pre_middle)).astype(jnp.bfloat16)
    raw_middle = jnp.dot(act_first.T, slope_middle, preferred_element_type=jnp.float32)
    back_first = jnp.dot(slope_middle, w_middle.T, preferred_element_type=jnp.float32)
    slope_first = (back_first * silu_slope(pre_first)).astype(jnp.bfloat16)
    raw_first = jnp.dot(belief.T, slope_first, preferred_element_type=jnp.float32)
    return (raw_first, raw_middle, raw_last)

def reference(belief, target_value, counts, w_first, w_middle, w_last):
    total_rows = belief.shape[0]
    span_rows = SUB_DEV * BLOCK
    block_count = total_rows // span_rows
    live_all = (counts[:, None] > jnp.arange(BLOCK, dtype=jnp.int32)[None, :]).astype(jnp.float32).reshape(total_rows)

    def add_block(running, block_index):
        row_start = (block_index * span_rows).astype(jnp.int32)
        part_belief = lax.dynamic_slice_in_dim(belief, row_start, span_rows, 0)
        part_target = lax.dynamic_slice_in_dim(target_value, row_start, span_rows, 0)
        part_live = lax.dynamic_slice_in_dim(live_all, row_start, span_rows, 0)
        pieces = rows_grads(part_belief, part_target, part_live, w_first, w_middle, w_last)
        return (tuple((left + right for left, right in zip(running, pieces))), None)
    zeros_init = (jnp.zeros(w_first.shape, jnp.float32), jnp.zeros(w_middle.shape, jnp.float32), jnp.zeros(w_last.shape, jnp.float32))
    running, _ = lax.scan(add_block, zeros_init, jnp.arange(block_count, dtype=jnp.int32))
    raw_first, raw_middle, raw_last = running
    square_sum = jnp.sum(raw_first * raw_first) + jnp.sum(raw_middle * raw_middle) + jnp.sum(raw_last * raw_last)
    norm_scale = lax.rsqrt(square_sum / PARAMS + 1e-06)
    return (raw_first * norm_scale, raw_middle * norm_scale, raw_last * norm_scale)
```

```python
import functools

import jax
import jax.numpy as jnp
from jax import lax
from jax.experimental import pallas as pl
from jax.experimental.pallas import tpu as pltpu
from jax.sharding import PartitionSpec as P

BLOCK = 128
LANES = 128
MESH = pl.DeviceIdType.MESH


def silu_slope(pre_act):
    sigmoid_of = jax.nn.sigmoid(pre_act)
    return sigmoid_of * (1.0 + pre_act * (1.0 - sigmoid_of))


def pad_to(size, step):
    return -(-size // step) * step


def cut_pieces(shapes, cuts):
    pairs = []
    for which, parts in cuts:
        tiles = shapes[which][-1] // LANES
        bounds = [round(tiles * i / (2 * parts)) * LANES for i in range(2 * parts + 1)]
        for i in range(parts):
            pairs.append(
                tuple(
                    (which, bounds[2 * i + t], bounds[2 * i + t + 1] - bounds[2 * i + t])
                    for t in range(2)
                )
            )
    return pairs


def scatter_kernel(dims, params, pairs, *refs):
    n_dp, n_mp = dims
    far = n_dp // 4
    count = len(pairs)
    flat = 2 * count
    grads, outs = refs[:3], refs[3:6]
    got1, sum1, got2, sum2, got3 = (refs[6 + k * flat : 6 + (k + 1) * flat] for k in range(5))
    sq_send, sq_got, send_sems, got_sems, far_send, far_got, sq_sems = refs[6 + 5 * flat :]

    dp, mp = lax.axis_index("dp"), lax.axis_index("mp")
    low, mid, top = dp % 2, (dp // 2) % 2, dp // 4
    me = dp * n_mp + mp
    total = n_dp * n_mp

    barrier = pltpu.get_barrier_semaphore()

    def greet(j, _):
        other = lax.rem(me + j, total)
        pl.semaphore_signal(
            barrier, inc=1, device_id=(other // n_mp, other % n_mp), device_id_type=MESH
        )
        return 0

    lax.fori_loop(1, total, greet, 0)
    pl.semaphore_wait(barrier, total - 1)

    low_peer = (dp + 1 - 2 * low, mp)
    mid_peer = (dp + 2 - 4 * mid, mp)

    def copy1(p, t):
        which, start, width = pairs[p][t]
        cols = pl.ds(start, width)
        src = (
            grads[which].at[:, :, 1 - low, :, cols]
            if t == 0
            else grads[which].at[:, 1 - mid, :, :, cols]
        )
        k = 2 * p + t
        return pltpu.make_async_remote_copy(
            src, got1[k], send_sems.at[0, k], got_sems.at[0, k],
            device_id=low_peer if t == 0 else mid_peer, device_id_type=MESH,
        )

    def copy2(p, t):
        k = 2 * p + t
        return pltpu.make_async_remote_copy(
            sum1[k].at[:, (1 - mid) if t == 0 else (1 - low)], got2[k],
            send_sems.at[1, k], got_sems.at[1, k],
            device_id=mid_peer if t == 0 else low_peer, device_id_type=MESH,
        )

    def copy3(p, t, j):
        k = 2 * p + t
        goal = lax.rem(top + j, far)
        return pltpu.make_async_remote_copy(
            sum2[k].at[goal], got3[k].at[j - 1], far_send.at[k, j - 1], far_got.at[k, j - 1],
            device_id=(dp + (goal - top) * 4, mp), device_id_type=MESH,
        )

    def add1(p, t):
        which, start, width = pairs[p][t]
        k = 2 * p + t

        def body(i, _):
            z, b = i // 2, i % 2
            own = (
                grads[which][z, b, low, :, start : start + width]
                if t == 0
                else grads[which][z, mid, b, :, start : start + width]
            )
            both = own.astype(jnp.float32) + got1[k][z, b].astype(jnp.float32)
            sum1[k][z, b] = both.astype(jnp.bfloat16)
            return 0

        lax.fori_loop(0, 2 * far, body, 0)

    def add2(p, t):
        k = 2 * p + t
        side = mid if t == 0 else low

        def body(z, _):
            both = sum1[k][z, side].astype(jnp.float32) + got2[k][z].astype(jnp.float32)
            sum2[k][z] = both.astype(jnp.bfloat16)
            return 0

        lax.fori_loop(0, far, body, 0)

    for p in range(min(2, count)):
        for t in range(2):
            copy1(p, t).start()
    for i in range(count + 1):
        if i < count:
            for t in range(2):
                copy1(i, t).wait_recv()
                add1(i, t)
                copy2(i, t).start()
            if i + 2 < count:
                for t in range(2):
                    copy1(i + 2, t).start()
        if i >= 1:
            for t in range(2):
                copy2(i - 1, t).wait_recv()
                add2(i - 1, t)
                for j in range(1, far):
                    copy3(i - 1, t, j).start()
    squares = jnp.float32(0.0)
    for p in range(count):
        for t in range(2):
            which, start, width = pairs[p][t]
            k = 2 * p + t
            value = sum2[k][top].astype(jnp.float32)
            for j in range(1, far):
                copy3(p, t, j).wait_recv()
                value = value + got3[k][j - 1].astype(jnp.float32)
            outs[which][:, start : start + width] = value
            squares = squares + jnp.sum(value * value)

    sq_send[...] = jnp.full(sq_send.shape, squares, jnp.float32)

    def share_copy(j):
        other = lax.rem(me + j, total)
        return pltpu.make_async_remote_copy(
            sq_send, sq_got.at[j - 1], sq_sems.at[0], sq_sems.at[1],
            device_id=(other // n_mp, other % n_mp), device_id_type=MESH,
        )

    def share(j, _):
        share_copy(j).start()
        return 0

    lax.fori_loop(1, total, share, 0)
    pltpu.make_async_copy(sq_got, sq_got, sq_sems.at[1]).wait()
    everyone = squares + jnp.sum(sq_got[...]) * (1.0 / (sq_send.shape[0] * sq_send.shape[1]))
    scale = lax.rsqrt(jnp.full((1, LANES), everyone / params + 1e-06, jnp.float32))
    for p in range(count):
        for t in range(2):
            which, start, width = pairs[p][t]
            for c in range(start, start + width, LANES):
                outs[which][:, c : c + LANES] = outs[which][:, c : c + LANES] * scale

    for p in range(count):
        for t in range(2):
            copy1(p, t).wait_send()
            copy2(p, t).wait_send()
            for j in range(1, far):
                copy3(p, t, j).wait_send()
    pltpu.make_async_copy(sq_got, sq_got, sq_sems.at[0]).wait()


def scatter_grads(dims, params, grads, cuts):
    n_dp, n_mp = dims
    far = n_dp // 4
    grads = [
        jnp.pad(g.astype(jnp.bfloat16), ((0, 0), (0, pad_to(g.shape[1], LANES) - g.shape[1])))
        .reshape(far, 2, 2, g.shape[0] // n_dp, pad_to(g.shape[1], LANES))
        for g in grads
    ]
    shapes = [g.shape for g in grads]
    pairs = cut_pieces(shapes, cuts)

    def buffers(lead):
        return [
            pltpu.VMEM(lead + (shapes[piece[0]][3], piece[2]), jnp.bfloat16)
            for pair in pairs
            for piece in pair
        ]

    flat = 2 * len(pairs)
    spec = pl.BlockSpec(memory_space=pltpu.VMEM)
    return pl.pallas_call(
        functools.partial(scatter_kernel, dims, params, pairs),
        out_shape=[jax.ShapeDtypeStruct(s[3:], jnp.float32) for s in shapes],
        in_specs=[spec] * 3,
        out_specs=[spec] * 3,
        scratch_shapes=(
            buffers((far, 2)) + buffers((far, 2)) + buffers((far,)) + buffers((far,))
            + buffers((far - 1,))
            + [
                pltpu.VMEM((8, LANES), jnp.float32),
                pltpu.VMEM((n_dp * n_mp - 1, 8, LANES), jnp.float32),
                pltpu.SemaphoreType.DMA((2, flat)),
                pltpu.SemaphoreType.DMA((2, flat)),
                pltpu.SemaphoreType.DMA((flat, far - 1)),
                pltpu.SemaphoreType.DMA((flat, far - 1)),
                pltpu.SemaphoreType.DMA((2,)),
            ]
        ),
        compiler_params=pltpu.CompilerParams(
            collective_id=0, has_side_effects=True, vmem_limit_bytes=60 * 1024 * 1024
        ),
    )(*grads)


def per_device(dims, belief, target_value, counts, w_first, w_middle, w_last):
    n_dp, n_mp = dims
    total_rows = belief.shape[0]
    own_width = w_last.shape[1]
    params = float(n_mp * (w_first.size + w_middle.size + w_last.size))
    target_value = lax.dynamic_slice_in_dim(
        target_value, lax.axis_index("mp") * own_width, own_width, 1
    )
    live_rows = (counts[:, None] > jnp.arange(BLOCK, dtype=jnp.int32)[None, :]).reshape(total_rows)
    live_mask = live_rows.astype(jnp.float32)

    pre_first = jnp.dot(belief, w_first, preferred_element_type=jnp.float32)
    act_first = jax.nn.silu(pre_first).astype(jnp.bfloat16)
    partial_middle = jnp.dot(act_first, w_middle, preferred_element_type=jnp.float32)
    pre_middle = lax.psum(partial_middle, "mp")
    act_middle = jax.nn.silu(pre_middle).astype(jnp.bfloat16)
    predicted = jnp.dot(act_middle, w_last, preferred_element_type=jnp.float32)
    mismatch = predicted - target_value.astype(jnp.float32)
    slope_out = (jnp.clip(mismatch, -1.0, 1.0) * live_mask[:, None]).astype(jnp.bfloat16)
    raw_last = jnp.dot(act_middle.T, slope_out, preferred_element_type=jnp.float32)
    partial_back = jnp.dot(slope_out, w_last.T, preferred_element_type=jnp.float32)
    back_middle = lax.psum(partial_back, "mp")
    slope_middle = (back_middle * silu_slope(pre_middle)).astype(jnp.bfloat16)
    raw_middle = jnp.dot(slope_middle.T, act_first, preferred_element_type=jnp.float32)
    back_first = jnp.dot(slope_middle, w_middle.T, preferred_element_type=jnp.float32)
    slope_first = (back_first * silu_slope(pre_first)).astype(jnp.bfloat16)
    raw_first = jnp.dot(slope_first.T, belief, preferred_element_type=jnp.float32)

    first, middle, last = scatter_grads(
        dims, params, (raw_first, raw_middle, raw_last), ((2, 1), (1, 1), (0, 2))
    )
    return first[:, : belief.shape[1]].T, middle.T, last[:, :own_width]


def solution(mesh):
    return jax.shard_map(
        functools.partial(per_device, (mesh.shape["dp"], mesh.shape["mp"])),
        mesh=mesh,
        in_specs=(
            P("dp", None),
            P("dp", None),
            P("dp"),
            P(None, "mp"),
            P("mp", None),
            P(None, "mp"),
        ),
        out_specs=(P(None, ("mp", "dp")), P("mp", "dp"), P("dp", "mp")),
        check_vma=False,
    )
```

```python
import functools

import jax
import jax.numpy as jnp
from jax import lax
from jax.experimental import pallas as pl
from jax.experimental.pallas import tpu as pltpu
from jax.sharding import PartitionSpec as P

BLOCK = 128
LANES = 128
MESH = pl.DeviceIdType.MESH


def silu_slope(pre_act):
    sigmoid_of = jax.nn.sigmoid(pre_act)
    return sigmoid_of * (1.0 + pre_act * (1.0 - sigmoid_of))


def pad_to(size, step):
    return -(-size // step) * step


def cut_pieces(shapes, cuts):
    pairs = []
    for which, parts in cuts:
        tiles = shapes[which][-1] // LANES
        bounds = [round(tiles * i / (2 * parts)) * LANES for i in range(2 * parts + 1)]
        for i in range(parts):
            pairs.append(
                tuple(
                    (which, bounds[2 * i + t], bounds[2 * i + t + 1] - bounds[2 * i + t])
                    for t in range(2)
                )
            )
    return pairs


def step_kernel(dims, params, pairs, blocks, *refs):
    n_dp, n_mp = dims
    far = n_dp // 4
    count = len(pairs)
    flat = 2 * count
    counts, loads, outs = refs[0], refs[1:6], refs[6:9]
    refs = refs[9:]
    got1, sum1, got2, sum2, got3 = (refs[k * flat : (k + 1) * flat] for k in range(5))
    refs = refs[5 * flat :]
    held, grads = refs[:5], refs[5:8]
    (
        pre1, act1, slope1_t, part2, other2, pre2, act2, act2_t, slope_last, part_back, other_back,
        slope2, slope2_t, load_sems, swap_send, swap_got,
        sq_send, sq_got, send_sems, got_sems, far_send, far_got, sq_sems,
    ) = refs[8:]
    belief, target, w_first, w_middle, w_last = held
    arrivals = [
        pltpu.make_async_copy(src, dst, load_sems.at[i])
        for i, (src, dst) in enumerate(zip(loads, held))
    ]
    for i in (0, 2, 3, 4, 1):
        arrivals[i].start()

    dp, mp = lax.axis_index("dp"), lax.axis_index("mp")
    low, mid, top = dp % 2, (dp // 2) % 2, dp // 4
    me = dp * n_mp + mp
    total = n_dp * n_mp

    barrier = pltpu.get_barrier_semaphore()

    def greet(j, _):
        other = lax.rem(me + j, total)
        pl.semaphore_signal(
            barrier, inc=1, device_id=(other // n_mp, other % n_mp), device_id_type=MESH
        )
        return 0

    lax.fori_loop(1, total, greet, 0)
    pl.semaphore_wait(barrier, total - 1)

    low_peer = (dp + 1 - 2 * low, mp)
    mid_peer = (dp + 2 - 4 * mid, mp)

    def copy1(p, t):
        which, start, width = pairs[p][t]
        cols = pl.ds(start, width)
        src = (
            grads[which].at[:, :, 1 - low, :, cols]
            if t == 0
            else grads[which].at[:, 1 - mid, :, :, cols]
        )
        k = 2 * p + t
        return pltpu.make_async_remote_copy(
            src, got1[k], send_sems.at[0, k], got_sems.at[0, k],
            device_id=low_peer if t == 0 else mid_peer, device_id_type=MESH,
        )

    def copy2(p, t):
        k = 2 * p + t
        return pltpu.make_async_remote_copy(
            sum1[k].at[:, (1 - mid) if t == 0 else (1 - low)], got2[k],
            send_sems.at[1, k], got_sems.at[1, k],
            device_id=mid_peer if t == 0 else low_peer, device_id_type=MESH,
        )

    def copy3(p, t, j):
        k = 2 * p + t
        goal = lax.rem(top + j, far)
        return pltpu.make_async_remote_copy(
            sum2[k].at[goal], got3[k].at[j - 1], far_send.at[k, j - 1], far_got.at[k, j - 1],
            device_id=(dp + (goal - top) * 4, mp), device_id_type=MESH,
        )

    def add1(p, t):
        which, start, width = pairs[p][t]
        k = 2 * p + t

        def body(i, _):
            z, b = i // 2, i % 2
            own = (
                grads[which][z, b, low, :, start : start + width]
                if t == 0
                else grads[which][z, mid, b, :, start : start + width]
            )
            both = own.astype(jnp.float32) + got1[k][z, b].astype(jnp.float32)
            sum1[k][z, b] = both.astype(jnp.bfloat16)
            return 0

        lax.fori_loop(0, 2 * far, body, 0)

    def add2(p, t):
        k = 2 * p + t
        side = mid if t == 0 else low

        def body(z, _):
            both = sum1[k][z, side].astype(jnp.float32) + got2[k][z].astype(jnp.float32)
            sum2[k][z] = both.astype(jnp.bfloat16)
            return 0

        lax.fori_loop(0, far, body, 0)

    rows, hid = act2.shape
    own_width = w_last.shape[1]
    in_width = belief.shape[1]
    block = hid // blocks

    def swap(side, part, other, i):
        return pltpu.make_async_remote_copy(
            part.at[i], other.at[i], swap_send.at[side, i], swap_got.at[side, i],
            device_id=(dp, 1 - mp), device_id_type=MESH,
        )

    def weight_grad(which, left_t, right, stop, start, width):
        r = grads[which].shape[3]
        real = min(width, stop - start)

        def body(z, _):
            at = pl.multiple_of(z * 4 * r, 16)
            value = jnp.dot(
                left_t[pl.ds(at, 4 * r), :], right[:, start : start + real],
                preferred_element_type=jnp.float32,
            )
            if real < width:
                value = jnp.concatenate(
                    [value, jnp.zeros((4 * r, width - real), jnp.float32)], axis=1
                )
            for b in range(4):
                grads[which][z, b // 2, b % 2, :, start : start + width] = value[
                    b * r : (b + 1) * r
                ].astype(jnp.bfloat16)
            return 0

        lax.fori_loop(0, far, body, 0)

    def pair_grads(p, left_t, right, stop):
        for t in range(2):
            which, start, width = pairs[p][t]
            weight_grad(which, left_t, right, stop, start, width)
            copy1(p, t).start()

    own_hid = act1.shape[1]
    arrivals[0].wait()
    arrivals[2].wait()
    for c in range(0, own_hid, 256):
        value = jnp.dot(
            belief[...], w_first[:, c : c + 256], preferred_element_type=jnp.float32
        )
        pre1[:, c : c + 256] = value
        act1[:, c : c + 256] = jax.nn.silu(value).astype(jnp.bfloat16)
    arrivals[3].wait()
    for i in range(blocks):
        part2[i] = jnp.dot(
            act1[...], w_middle[:, i * block : (i + 1) * block],
            preferred_element_type=jnp.float32,
        )
        swap(0, part2, other2, i).start()
    arrivals[1].wait()
    arrivals[4].wait()
    row = lax.broadcasted_iota(jnp.int32, (rows, 1), 0)
    limit = jnp.full((rows, 1), counts[0], jnp.int32)
    for b in range(1, rows // BLOCK):
        limit = jnp.where(row >= b * BLOCK, counts[b] + b * BLOCK, limit)
    live = jnp.where(row < limit, 1.0, 0.0)
    for i in range(blocks):
        cols = slice(i * block, (i + 1) * block)
        swap(0, part2, other2, i).wait_recv()
        value = part2[i] + other2[i]
        pre2[:, cols] = value
        act = jax.nn.silu(value)
        act2[:, cols] = act.astype(jnp.bfloat16)
        act2_t[cols, :] = act.astype(jnp.bfloat16).T
    wanted = target[:, :own_width].astype(jnp.float32)
    for m in range(1, n_mp):
        wanted = jnp.where(
            mp == m, target[:, m * own_width : (m + 1) * own_width].astype(jnp.float32), wanted
        )
    predicted = jnp.dot(act2[...], w_last[...], preferred_element_type=jnp.float32)
    slope_last[...] = (jnp.clip(predicted - wanted, -1.0, 1.0) * live).astype(jnp.bfloat16)
    for i in range(blocks):
        part_back[i] = lax.dot_general(
            slope_last[...], w_last[i * block : (i + 1) * block, :], (((1,), (1,)), ((), ())),
            preferred_element_type=jnp.float32,
        )
        swap(1, part_back, other_back, i).start()
    for p in range(count):
        if pairs[p][0][0] == 2:
            pair_grads(p, act2_t, slope_last, own_width)
    for i in range(blocks):
        cols = slice(i * block, (i + 1) * block)
        swap(1, part_back, other_back, i).wait_recv()
        value = (part_back[i] + other_back[i]) * silu_slope(pre2[:, cols])
        slope2[:, cols] = value.astype(jnp.bfloat16)
        slope2_t[cols, :] = value.astype(jnp.bfloat16).T
    for p in range(count):
        if pairs[p][0][0] == 1:
            pair_grads(p, slope2_t, act1, own_hid)
    for c in range(0, own_hid, 256):
        back = lax.dot_general(
            slope2[...], w_middle[c : c + 256, :], (((1,), (1,)), ((), ())),
            preferred_element_type=jnp.float32,
        )
        value = back * silu_slope(pre1[:, c : c + 256])
        slope1_t[c : c + 256, :] = value.astype(jnp.bfloat16).T
    for i in range(blocks):
        swap(0, part2, other2, i).wait_send()
        swap(1, part_back, other_back, i).wait_send()

    def first_grads(p):
        if pairs[p][0][0] == 0:
            pair_grads(p, slope1_t, belief, in_width)

    for p in range(min(3, count)):
        first_grads(p)
    for i in range(count + 1):
        if i < count:
            for t in range(2):
                copy1(i, t).wait_recv()
                add1(i, t)
                copy2(i, t).start()
            if i + 3 < count:
                first_grads(i + 3)
        if i >= 1:
            for t in range(2):
                copy2(i - 1, t).wait_recv()
                add2(i - 1, t)
                for j in range(1, far):
                    copy3(i - 1, t, j).start()
    squares = jnp.float32(0.0)
    for p in range(count):
        for t in range(2):
            which, start, width = pairs[p][t]
            k = 2 * p + t
            value = sum2[k][top].astype(jnp.float32)
            for j in range(1, far):
                copy3(p, t, j).wait_recv()
                value = value + got3[k][j - 1].astype(jnp.float32)
            outs[which][:, start : start + width] = value
            squares = squares + jnp.sum(value * value)

    sq_send[...] = jnp.full(sq_send.shape, squares, jnp.float32)

    def share_copy(j):
        other = lax.rem(me + j, total)
        return pltpu.make_async_remote_copy(
            sq_send, sq_got.at[j - 1], sq_sems.at[0], sq_sems.at[1],
            device_id=(other // n_mp, other % n_mp), device_id_type=MESH,
        )

    def share(j, _):
        share_copy(j).start()
        return 0

    lax.fori_loop(1, total, share, 0)
    pltpu.make_async_copy(sq_got, sq_got, sq_sems.at[1]).wait()
    everyone = squares + jnp.sum(sq_got[...]) * (1.0 / (sq_send.shape[0] * sq_send.shape[1]))
    scale = lax.rsqrt(jnp.full((1, LANES), everyone / params + 1e-06, jnp.float32))
    for p in range(count):
        for t in range(2):
            which, start, width = pairs[p][t]
            for c in range(start, start + width, LANES):
                outs[which][:, c : c + LANES] = outs[which][:, c : c + LANES] * scale

    for p in range(count):
        for t in range(2):
            copy1(p, t).wait_send()
            copy2(p, t).wait_send()
            for j in range(1, far):
                copy3(p, t, j).wait_send()
    pltpu.make_async_copy(sq_got, sq_got, sq_sems.at[0]).wait()


def per_device(dims, belief, target_value, counts, w_first, w_middle, w_last):
    n_dp, n_mp = dims
    far = n_dp // 4
    blocks = 3
    rows, (in_width, own_hid) = belief.shape[0], w_first.shape
    hid, own_width = w_last.shape
    params = float(n_mp * (w_first.size + w_middle.size + w_last.size))
    shapes = [
        (far, 2, 2, long // n_dp, pad_to(wide, LANES))
        for long, wide in ((own_hid, in_width), (hid, own_hid), (hid, own_width))
    ]
    pairs = cut_pieces(shapes, ((2, 1), (1, 1), (0, 2)))

    def buffers(lead):
        return [
            pltpu.VMEM(lead + (shapes[piece[0]][3], piece[2]), jnp.bfloat16)
            for pair in pairs
            for piece in pair
        ]

    flat = 2 * len(pairs)
    loads = (belief, target_value, w_first, w_middle, w_last)
    swapped = pltpu.VMEM((blocks, rows, hid // blocks), jnp.float32)
    half, single = jnp.bfloat16, jnp.float32
    first, middle, last = pl.pallas_call(
        functools.partial(step_kernel, dims, params, pairs, blocks),
        out_shape=[jax.ShapeDtypeStruct(s[3:], jnp.float32) for s in shapes],
        in_specs=[pl.BlockSpec(memory_space=pltpu.SMEM)]
        + [pl.BlockSpec(memory_space=pl.ANY)] * 5,
        out_specs=[pl.BlockSpec(memory_space=pltpu.VMEM)] * 3,
        scratch_shapes=(
            buffers((far, 2)) + buffers((far, 2)) + buffers((far,)) + buffers((far,))
            + buffers((far - 1,))
            + [pltpu.VMEM(x.shape, x.dtype) for x in loads]
            + [pltpu.VMEM(s, half) for s in shapes]
            + [
                pltpu.VMEM((rows, own_hid), single),
                pltpu.VMEM((rows, own_hid), half),
                pltpu.VMEM((own_hid, rows), half),
                swapped,
                swapped,
                pltpu.VMEM((rows, hid), single),
                pltpu.VMEM((rows, hid), half),
                pltpu.VMEM((hid, rows), half),
                pltpu.VMEM((rows, own_width), half),
                swapped,
                swapped,
                pltpu.VMEM((rows, hid), half),
                pltpu.VMEM((hid, rows), half),
                pltpu.SemaphoreType.DMA((5,)),
                pltpu.SemaphoreType.DMA((2, blocks)),
                pltpu.SemaphoreType.DMA((2, blocks)),
                pltpu.VMEM((8, LANES), jnp.float32),
                pltpu.VMEM((n_dp * n_mp - 1, 8, LANES), jnp.float32),
                pltpu.SemaphoreType.DMA((2, flat)),
                pltpu.SemaphoreType.DMA((2, flat)),
                pltpu.SemaphoreType.DMA((flat, far - 1)),
                pltpu.SemaphoreType.DMA((flat, far - 1)),
                pltpu.SemaphoreType.DMA((2,)),
            ]
        ),
        compiler_params=pltpu.CompilerParams(
            collective_id=0, has_side_effects=True, vmem_limit_bytes=60 * 1024 * 1024
        ),
    )(counts, *loads)
    return first[:, :in_width].T, middle.T, last[:, :own_width]


def solution(mesh):
    return jax.shard_map(
        functools.partial(per_device, (mesh.shape["dp"], mesh.shape["mp"])),
        mesh=mesh,
        in_specs=(
            P("dp", None),
            P("dp", None),
            P("dp"),
            P(None, "mp"),
            P("mp", None),
            P(None, "mp"),
        ),
        out_specs=(P(None, ("mp", "dp")), P("mp", "dp"), P("dp", "mp")),
        check_vma=False,
    )
```

```python
import functools

import jax
import jax.numpy as jnp
from jax import lax
from jax.experimental import pallas as pl
from jax.experimental.pallas import tpu as pltpu
from jax.sharding import PartitionSpec as P

BLOCK = 128
LANES = 128
MESH = pl.DeviceIdType.MESH


def silu_slope(pre_act):
    sigmoid_of = jax.nn.sigmoid(pre_act)
    return sigmoid_of * (1.0 + pre_act * (1.0 - sigmoid_of))


def pad_to(size, step):
    return -(-size // step) * step


def cut_pieces(shapes, cuts):
    pairs = []
    for which, parts in cuts:
        tiles = shapes[which][-1] // LANES
        bounds = [round(tiles * i / (2 * parts)) * LANES for i in range(2 * parts + 1)]
        for i in range(parts):
            pairs.append(
                tuple(
                    (which, bounds[2 * i + t], bounds[2 * i + t + 1] - bounds[2 * i + t])
                    for t in range(2)
                )
            )
    return pairs


def step_kernel(dims, params, pairs, blocks, *refs):
    n_dp, n_mp = dims
    far = n_dp // 4
    count = len(pairs)
    flat = 2 * count
    counts, loads, outs = refs[0], refs[1:6], refs[6:9]
    refs = refs[9:]
    got1, sum1, got2, sum2, got3 = (refs[k * flat : (k + 1) * flat] for k in range(5))
    refs = refs[5 * flat :]
    held, grads = refs[:5], refs[5:8]
    (
        pre1, act1, slope1_t, part2, other2, pre2, act2, act2_t, slope_last, part_back, other_back,
        slope2, slope2_t, load_sems, swap_send, swap_got,
        sq_send, sq_got, send_sems, got_sems, far_send, far_got, sq_sems,
    ) = refs[8:]
    belief, target, w_first, w_middle, w_last = held
    arrivals = [
        pltpu.make_async_copy(src, dst, load_sems.at[i])
        for i, (src, dst) in enumerate(zip(loads, held))
    ]
    for i in (0, 2, 3, 4, 1):
        arrivals[i].start()

    dp, mp = lax.axis_index("dp"), lax.axis_index("mp")
    low, mid, top = dp % 2, (dp // 2) % 2, dp // 4
    me = dp * n_mp + mp
    total = n_dp * n_mp

    barrier = pltpu.get_barrier_semaphore()

    def greet(j, _):
        other = lax.rem(me + j, total)
        pl.semaphore_signal(
            barrier, inc=1, device_id=(other // n_mp, other % n_mp), device_id_type=MESH
        )
        return 0

    lax.fori_loop(1, total, greet, 0)
    pl.semaphore_wait(barrier, total - 1)

    low_peer = (dp + 1 - 2 * low, mp)
    mid_peer = (dp + 2 - 4 * mid, mp)

    def copy1(p, t):
        which, start, width = pairs[p][t]
        cols = pl.ds(start, width)
        src = (
            grads[which].at[:, :, 1 - low, :, cols]
            if t == 0
            else grads[which].at[:, 1 - mid, :, :, cols]
        )
        k = 2 * p + t
        return pltpu.make_async_remote_copy(
            src, got1[k], send_sems.at[0, k], got_sems.at[0, k],
            device_id=low_peer if t == 0 else mid_peer, device_id_type=MESH,
        )

    def copy2(p, t):
        k = 2 * p + t
        return pltpu.make_async_remote_copy(
            sum1[k].at[:, (1 - mid) if t == 0 else (1 - low)], got2[k],
            send_sems.at[1, k], got_sems.at[1, k],
            device_id=mid_peer if t == 0 else low_peer, device_id_type=MESH,
        )

    def copy3(p, t, j):
        k = 2 * p + t
        goal = lax.rem(top + j, far)
        return pltpu.make_async_remote_copy(
            sum2[k].at[goal], got3[k].at[j - 1], far_send.at[k, j - 1], far_got.at[k, j - 1],
            device_id=(dp + (goal - top) * 4, mp), device_id_type=MESH,
        )

    def add1(p, t):
        which, start, width = pairs[p][t]
        k = 2 * p + t

        def body(i, _):
            z, b = i // 2, i % 2
            own = (
                grads[which][z, b, low, :, start : start + width]
                if t == 0
                else grads[which][z, mid, b, :, start : start + width]
            )
            both = own.astype(jnp.float32) + got1[k][z, b].astype(jnp.float32)
            sum1[k][z, b] = both.astype(jnp.bfloat16)
            return 0

        lax.fori_loop(0, 2 * far, body, 0)

    def add2(p, t):
        k = 2 * p + t
        side = mid if t == 0 else low

        def body(z, _):
            both = sum1[k][z, side].astype(jnp.float32) + got2[k][z].astype(jnp.float32)
            sum2[k][z] = both.astype(jnp.bfloat16)
            return 0

        lax.fori_loop(0, far, body, 0)

    rows, hid = act2.shape
    own_width = w_last.shape[1]
    in_width = belief.shape[1]
    block = hid // blocks

    def swap(side, part, other, i):
        return pltpu.make_async_remote_copy(
            part.at[i], other.at[i], swap_send.at[side, i], swap_got.at[side, i],
            device_id=(dp, 1 - mp), device_id_type=MESH,
        )

    def weight_grad(which, left_t, right, stop, start, width):
        r = grads[which].shape[3]
        real = min(width, stop - start)

        def body(z, _):
            at = pl.multiple_of(z * 4 * r, 16)
            value = jnp.dot(
                left_t[pl.ds(at, 4 * r), :], right[:, start : start + real],
                preferred_element_type=jnp.float32,
            )
            if real < width:
                value = jnp.concatenate(
                    [value, jnp.zeros((4 * r, width - real), jnp.float32)], axis=1
                )
            for b in range(4):
                grads[which][z, b // 2, b % 2, :, start : start + width] = value[
                    b * r : (b + 1) * r
                ].astype(jnp.bfloat16)
            return 0

        lax.fori_loop(0, far, body, 0)

    def pair_grads(p, left_t, right, stop):
        for t in range(2):
            which, start, width = pairs[p][t]
            weight_grad(which, left_t, right, stop, start, width)
            copy1(p, t).start()

    own_hid = act1.shape[1]
    arrivals[0].wait()
    arrivals[2].wait()
    for c in range(0, own_hid, 256):
        value = jnp.dot(
            belief[...], w_first[:, c : c + 256], preferred_element_type=jnp.float32
        )
        pre1[:, c : c + 256] = value
        act1[:, c : c + 256] = jax.nn.silu(value).astype(jnp.bfloat16)
    arrivals[3].wait()
    for i in range(blocks):
        part2[i] = jnp.dot(
            act1[...], w_middle[:, i * block : (i + 1) * block],
            preferred_element_type=jnp.float32,
        )
        swap(0, part2, other2, i).start()
    arrivals[1].wait()
    arrivals[4].wait()
    row = lax.broadcasted_iota(jnp.int32, (rows, 1), 0)
    limit = jnp.full((rows, 1), counts[0], jnp.int32)
    for b in range(1, rows // BLOCK):
        limit = jnp.where(row >= b * BLOCK, counts[b] + b * BLOCK, limit)
    live = jnp.where(row < limit, 1.0, 0.0)
    for i in range(blocks):
        cols = slice(i * block, (i + 1) * block)
        swap(0, part2, other2, i).wait_recv()
        value = part2[i] + other2[i]
        pre2[:, cols] = value
        act = jax.nn.silu(value)
        act2[:, cols] = act.astype(jnp.bfloat16)
        act2_t[cols, :] = act.astype(jnp.bfloat16).T
    wanted = target[:, :own_width].astype(jnp.float32)
    for m in range(1, n_mp):
        wanted = jnp.where(
            mp == m, target[:, m * own_width : (m + 1) * own_width].astype(jnp.float32), wanted
        )
    predicted = jnp.dot(act2[...], w_last[...], preferred_element_type=jnp.float32)
    slope_last[...] = (jnp.clip(predicted - wanted, -1.0, 1.0) * live).astype(jnp.bfloat16)
    for i in range(blocks):
        part_back[i] = lax.dot_general(
            slope_last[...], w_last[i * block : (i + 1) * block, :], (((1,), (1,)), ((), ())),
            preferred_element_type=jnp.float32,
        )
        swap(1, part_back, other_back, i).start()
    for p in range(count):
        if pairs[p][0][0] == 2:
            pair_grads(p, act2_t, slope_last, own_width)
    for i in range(blocks):
        cols = slice(i * block, (i + 1) * block)
        swap(1, part_back, other_back, i).wait_recv()
        value = (part_back[i] + other_back[i]) * silu_slope(pre2[:, cols])
        slope2[:, cols] = value.astype(jnp.bfloat16)
        slope2_t[cols, :] = value.astype(jnp.bfloat16).T
    for p in range(count):
        if pairs[p][0][0] == 1:
            pair_grads(p, slope2_t, act1, own_hid)
    for c in range(0, own_hid, 256):
        back = lax.dot_general(
            slope2[...], w_middle[c : c + 256, :], (((1,), (1,)), ((), ())),
            preferred_element_type=jnp.float32,
        )
        value = back * silu_slope(pre1[:, c : c + 256])
        slope1_t[c : c + 256, :] = value.astype(jnp.bfloat16).T
    for i in range(blocks):
        swap(0, part2, other2, i).wait_send()
        swap(1, part_back, other_back, i).wait_send()

    def first_grads(p):
        if pairs[p][0][0] == 0:
            pair_grads(p, slope1_t, belief, in_width)

    for p in range(min(3, count)):
        first_grads(p)
    for i in range(count + 1):
        if i < count:
            for t in range(2):
                copy1(i, t).wait_recv()
                add1(i, t)
                copy2(i, t).start()
            if i + 3 < count:
                first_grads(i + 3)
        if i >= 1:
            for t in range(2):
                copy2(i - 1, t).wait_recv()
                add2(i - 1, t)
                for j in range(1, far):
                    copy3(i - 1, t, j).start()
    squares = jnp.float32(0.0)
    for p in range(count):
        for t in range(2):
            which, start, width = pairs[p][t]
            k = 2 * p + t
            value = sum2[k][top].astype(jnp.float32)
            for j in range(1, far):
                copy3(p, t, j).wait_recv()
                value = value + got3[k][j - 1].astype(jnp.float32)
            outs[which][:, start : start + width] = value
            squares = squares + jnp.sum(value * value)

    sq_send[...] = jnp.full(sq_send.shape, squares, jnp.float32)

    def share_copy(j):
        other = lax.rem(me + j, total)
        return pltpu.make_async_remote_copy(
            sq_send, sq_got.at[j - 1], sq_sems.at[0], sq_sems.at[1],
            device_id=(other // n_mp, other % n_mp), device_id_type=MESH,
        )

    def share(j, _):
        share_copy(j).start()
        return 0

    lax.fori_loop(1, total, share, 0)
    pltpu.make_async_copy(sq_got, sq_got, sq_sems.at[1]).wait()
    everyone = squares + jnp.sum(sq_got[...]) * (1.0 / (sq_send.shape[0] * sq_send.shape[1]))
    scale = lax.rsqrt(jnp.full((1, LANES), everyone / params + 1e-06, jnp.float32))
    for p in range(count):
        for t in range(2):
            which, start, width = pairs[p][t]
            for c in range(start, start + width, LANES):
                outs[which][:, c : c + LANES] = outs[which][:, c : c + LANES] * scale

    for p in range(count):
        for t in range(2):
            copy1(p, t).wait_send()
            copy2(p, t).wait_send()
            for j in range(1, far):
                copy3(p, t, j).wait_send()
    pltpu.make_async_copy(sq_got, sq_got, sq_sems.at[0]).wait()


def per_device(dims, belief, target_value, counts, w_first, w_middle, w_last):
    n_dp, n_mp = dims
    far = n_dp // 4
    blocks = 3
    rows, (in_width, own_hid) = belief.shape[0], w_first.shape
    hid, own_width = w_last.shape
    params = float(n_mp * (w_first.size + w_middle.size + w_last.size))
    shapes = [
        (far, 2, 2, long // n_dp, pad_to(wide, LANES))
        for long, wide in ((own_hid, in_width), (hid, own_hid), (hid, own_width))
    ]
    pairs = cut_pieces(shapes, ((2, 1), (1, 1), (0, 4)))

    def buffers(lead):
        return [
            pltpu.VMEM(lead + (shapes[piece[0]][3], piece[2]), jnp.bfloat16)
            for pair in pairs
            for piece in pair
        ]

    flat = 2 * len(pairs)
    loads = (belief, target_value, w_first, w_middle, w_last)
    swapped = pltpu.VMEM((blocks, rows, hid // blocks), jnp.float32)
    half, single = jnp.bfloat16, jnp.float32
    first, middle, last = pl.pallas_call(
        functools.partial(step_kernel, dims, params, pairs, blocks),
        out_shape=[jax.ShapeDtypeStruct(s[3:], jnp.float32) for s in shapes],
        in_specs=[pl.BlockSpec(memory_space=pltpu.SMEM)]
        + [pl.BlockSpec(memory_space=pl.ANY)] * 5,
        out_specs=[pl.BlockSpec(memory_space=pltpu.VMEM)] * 3,
        scratch_shapes=(
            buffers((far, 2)) + buffers((far, 2)) + buffers((far,)) + buffers((far,))
            + buffers((far - 1,))
            + [pltpu.VMEM(x.shape, x.dtype) for x in loads]
            + [pltpu.VMEM(s, half) for s in shapes]
            + [
                pltpu.VMEM((rows, own_hid), single),
                pltpu.VMEM((rows, own_hid), half),
                pltpu.VMEM((own_hid, rows), half),
                swapped,
                swapped,
                pltpu.VMEM((rows, hid), single),
                pltpu.VMEM((rows, hid), half),
                pltpu.VMEM((hid, rows), half),
                pltpu.VMEM((rows, own_width), half),
                swapped,
                swapped,
                pltpu.VMEM((rows, hid), half),
                pltpu.VMEM((hid, rows), half),
                pltpu.SemaphoreType.DMA((5,)),
                pltpu.SemaphoreType.DMA((2, blocks)),
                pltpu.SemaphoreType.DMA((2, blocks)),
                pltpu.VMEM((8, LANES), jnp.float32),
                pltpu.VMEM((n_dp * n_mp - 1, 8, LANES), jnp.float32),
                pltpu.SemaphoreType.DMA((2, flat)),
                pltpu.SemaphoreType.DMA((2, flat)),
                pltpu.SemaphoreType.DMA((flat, far - 1)),
                pltpu.SemaphoreType.DMA((flat, far - 1)),
                pltpu.SemaphoreType.DMA((2,)),
            ]
        ),
        compiler_params=pltpu.CompilerParams(
            collective_id=0, has_side_effects=True, vmem_limit_bytes=60 * 1024 * 1024
        ),
    )(counts, *loads)
    return first[:, :in_width].T, middle.T, last[:, :own_width]


def solution(mesh):
    return jax.shard_map(
        functools.partial(per_device, (mesh.shape["dp"], mesh.shape["mp"])),
        mesh=mesh,
        in_specs=(
            P("dp", None),
            P("dp", None),
            P("dp"),
            P(None, "mp"),
            P("mp", None),
            P(None, "mp"),
        ),
        out_specs=(P(None, ("mp", "dp")), P("mp", "dp"), P("dp", "mp")),
        check_vma=False,
    )
```
